128 devices in a mesh: dp: 64 (over y, x, z), rep: 2 (over core).
Axes of the slice: x: 4, y: 4, z: 4, core: 2. Of those that a mesh axis runs over, the one named last changes fastest.
Arguments:
- row_grads: float32 [65536, 512], P(('dp', 'rep')), may hold values from -2500 to 2500
- token_owner: int32 [65536, 1], P(('dp', 'rep')), may hold values from 0 to 63; in each aligned block of 512 rows (0 to 511, 512 to 1023, ...) at most 16 rows name the same one
- token_row: int32 [65536], P(('dp', 'rep')), may hold values from 0 to 2047
- table: float32 [131072, 512], P('dp'), may hold values from -6 to 6
- moment: float32 [131072, 512], P('dp'), may hold values from -3 to 3
- second: float32 [131072, 512], P('dp'), may hold values from 0.05 to 2
Outputs:
- new_table: float32 [131072, 512], P('dp')
- new_moment: float32 [131072, 512], P('dp')
- new_second: float32 [131072, 512], P('dp')
The draws below stay inside these ranges and needn't reach their ends.
Inputs may be any that keep to these rules, and one draw needn't show every extreme that they name: `token_owner`: among the rows of one device at most 16 name one owner; in every draw some owner is named by exactly 16 rows of some device.
All inputs are finite; a program needn't handle non-finite values.
Results may differ from the reference program's by a relative error of at most 0.00007.
Values sent between devices are 32-bit elements; how exact they have to be, the bound alone decides.
No kernel may reach another device: no remote copies, remote signals or barrier semaphores. Data moves between devices by JAX's collectives and lax.ppermute only.
A program may use at most 128 MiB of HBM per device.

```python
import math
import jax
import jax.numpy as jnp
import numpy as np

VOCAB = 131072
ADAM_STEP = 100
TOK_DEV = 512
LW = 512
TOKENS = 65536
ROWS_OWN = 2048
CAP = 16
N_DP = 64
N_REP = 2


def draw_row_grads(key, part):
    keys = jax.random.split(key, 5)
    row_scale = jnp.exp(jax.random.uniform(keys[0], (TOKENS, 1), jnp.float32, 0.0, math.log(10.0)))
    col_scale = jnp.exp(jax.random.uniform(keys[1], (1, LW), jnp.float32, 0.0, math.log(10.0)))
    device_pos = (jnp.arange(TOKENS) // TOK_DEV).astype(jnp.float32)
    ramp = (1.0 + 2.0 * device_pos / max(N_DP * N_REP - 1, 1))[:, None]
    base = jnp.clip(jax.random.normal(keys[4], (TOKENS, LW), jnp.float32), -4.0, 4.0)
    return (base * row_scale * col_scale * ramp).astype(jnp.float32)


def place_ends(drawn, key, least, top_value):
    shape = drawn.shape
    spot = [jax.random.randint(jax.random.fold_in(key, axis), (), 0, shape[axis]) for axis in range(len(shape))]
    drawn = drawn.at[tuple(spot)].set(least)
    longest = shape.index(max(shape))
    spot[longest] = (spot[longest] + 1) % shape[longest]
    return drawn.at[tuple(spot)].set(top_value)


def steps_of(stream_key, shape, shards, least, top_value):
    loudness, own = 1.0, jax.random.fold_in(stream_key, 6)
    for axis_at, blocks in shards:
        heights = jnp.exp(jax.random.uniform(jax.random.fold_in(own, axis_at), (blocks,), jnp.float32, least / len(shards), top_value / len(shards)))
        loudness = loudness * jnp.repeat(heights, shape[axis_at] // blocks).reshape([-1 if axis == axis_at else 1 for axis in range(len(shape))])
    return loudness


def cumulative_ranks(number_of, slope):
    portions = [(1 << 20) // math.isqrt(grade ** slope) + 1 for grade in range(1, number_of + 1)]
    spread = 1 + sum(portions) // (1 << 30)
    return np.cumsum(np.array([max(1, weight // spread) for weight in portions]))


def skewed_ids(rng, shape, amount, lean):
    grid = cumulative_ranks(amount, lean)
    lot = jax.random.randint(jax.random.fold_in(rng, 1), shape, 0, int(grid[amount - 1]))
    grade = jnp.searchsorted(jnp.asarray(grid, jnp.int32), lot, side="right")
    return jax.random.permutation(jax.random.fold_in(rng, 2), amount)[grade].astype(jnp.int32)


def deal_out(stream_key, own, number, rows, count, top, most, lean):
    order = jax.random.permutation(stream_key, count)
    packed, usual = load_shares(count, rows * top, most, lean, True), load_shares(count, rows * top, most, lean, False)
    places = jnp.arange(count)

    def named(lengths, rotation):
        used = int((lengths > 0).sum())
        fixed = max(1, used // 4)
        moved = fixed + (places - fixed + rotation * (used - fixed)) % max(1, count - fixed)
        return jnp.zeros((count,), jnp.int32).at[order[jnp.where(places < fixed, places, moved)]].set(jnp.asarray(lengths, jnp.int32))

    lengths = jnp.where(number % 4 == 0, named(packed, number // 4), named(usual, number - number // 4 - 1))
    mixed = jax.random.permutation(jax.random.fold_in(own, 3), count)
    source_of, sink = mixed[0:count // 2 * 2:2], mixed[1:count // 2 * 2:2]
    slack = jnp.minimum(lengths[source_of] - 1, most - lengths[sink]) // 2
    slack = jnp.where((source_of == order[0]) | (sink == order[0]) | (lengths[sink] == 0), 0, jnp.maximum(slack, 0))
    moved = jax.random.randint(jax.random.fold_in(own, 4), (count // 2,), 0, 1 << 20) % (slack + 1)
    lengths = lengths.at[source_of].add(-moved).at[sink].add(moved)
    labels = jnp.searchsorted(jnp.cumsum(lengths), jnp.arange(rows * top), side="right").astype(jnp.int32)
    grid = labels.reshape(top, rows).T
    grid = grid[jax.random.permutation(jax.random.fold_in(own, 1), rows)]
    rotation = jax.random.randint(jax.random.fold_in(own, 2), (rows, 1), 0, top)
    return jnp.take_along_axis(grid, (jnp.arange(top)[None, :] + rotation) % top, axis=1)


def load_shares(amount, total, most, slope, full):
    weights = [(1 << 20) // math.isqrt(rank ** slope) + 1 for rank in range(1, amount + 1)]
    largest = most if full else min(most, max(-(-total // amount), total * weights[0] // sum(weights)))
    least = 1 if total - largest >= amount - 1 else 0
    holding, spare = [largest] + [least] * (amount - 1), total - largest - least * (amount - 1)
    while spare > 0:
        movable = [i for i in range(1, amount) if holding[i] < largest] or [i for i in range(1, amount) if holding[i] < most]
        pool, budget = sum([weights[i] for i in movable]), spare
        for i in movable:
            extra = min(most - holding[i], max(1, budget * weights[i] // pool), spare)
            holding[i] = holding[i] + extra
            spare = spare - extra
    return np.array(holding)


def noise(rng, dims, deviation, bound, pieces=(), kind=jnp.bfloat16):
    drawn = deviation * jax.random.normal(rng, dims, jnp.float32)
    if pieces:
        drawn = drawn * steps_of(rng, dims, pieces, -0.22, 0.18)
    return jnp.clip(drawn, -bound, bound).astype(kind)


def setup_inputs(seed: int = 0) -> dict:
    splits = jax.random.split(jax.random.key(seed), 7)
    row_grads = draw_row_grads(jax.random.fold_in(splits[6], 71), 0)
    token_owner_keys = jax.random.split(jax.random.fold_in(splits[1], 1), TOKENS // TOK_DEV)
    token_owner_turns = jax.random.permutation(jax.random.fold_in(splits[1], 3), TOKENS // TOK_DEV)
    token_owner = jax.vmap(lambda own, number: deal_out(jax.random.fold_in(splits[1], 2), own, number, TOK_DEV, N_DP, 1, CAP, 2))(token_owner_keys, token_owner_turns).reshape((TOKENS, 1))
    token_row = place_ends(skewed_ids(splits[2], (TOKENS,), ROWS_OWN, 2), jax.random.fold_in(splits[2], 3), 0, ROWS_OWN - 1).astype(jnp.int32)
    table = noise(splits[3], (VOCAB, LW), 1.0, 6.0, ((0, 64),), jnp.float32)
    moment = noise(splits[4], (VOCAB, LW), 0.5, 3.0, ((0, 64),), jnp.float32)
    second = jnp.clip(jnp.exp(math.log(2.0) - 3.6888794 * jax.random.uniform(splits[5], (VOCAB, LW), jnp.float32) ** steps_of(splits[5], (VOCAB, LW), ((0, 64),), -0.2, 0.2)), 0.05, 2.0)
    return {"row_grads": row_grads, "token_owner": token_owner, "token_row": token_row, "table": table, "moment": moment, "second": second}


def reference(row_grads, token_owner, token_row, table, moment, second):
    row_id = (token_owner[:, 0] * ROWS_OWN + token_row).astype(jnp.int32)
    dense = jnp.zeros((VOCAB, LW), jnp.float32).at[row_id].add(row_grads.astype(jnp.float32))
    norm = jnp.sqrt(jnp.sum(dense * dense))
    limit = 0.5 * jnp.sqrt(jnp.float32(VOCAB * LW))
    clip = jnp.minimum(jnp.float32(1.0), limit / (norm + 1e-06))
    clipped = clip * dense
    new_moment = 0.9 * moment + 0.1 * clipped
    new_second = 0.999 * second + 0.001 * clipped * clipped
    first_fix = 1.0 - 0.9 ** ADAM_STEP
    second_fix = 1.0 - 0.999 ** ADAM_STEP
    update = new_moment / first_fix / (jnp.sqrt(new_second / second_fix) + 1e-08)
    new_table = table - 0.01 * (update + 0.01 * table)
    return (new_table, new_moment, new_second)
```

```python
import jax
import jax.numpy as jnp
from jax import lax
from jax.experimental import pallas as pl
from jax.experimental.pallas import tpu as pltpu
from jax.sharding import PartitionSpec as P

VOCAB = 131072
ADAM_STEP = 100
LW = 512
OWNERS = 64
SLOTS = 16
TOKENS = 512
ROWS = 2048
DEVICES = 128
BLOCK = 2 * SLOTS + 1
PITCH = 2064
CHAINS = 4
CHUNK = 128
AXES = ("dp", "rep")
VMEM = pltpu.MemorySpace.VMEM
SMEM = pltpu.MemorySpace.SMEM


def pack_kernel(owner, row, x, send, ids_v, ids_s, sem):
    line = lax.broadcasted_iota(jnp.int32, (16, 128), 0)
    ids_v[...] = jnp.where(line < 8, ROWS, 0)
    copy = pltpu.make_async_copy(ids_v, ids_s, sem)
    copy.start()
    copy.wait()

    def tokens(step, _):
        for k in range(8):
            t = step * 8 + k
            o = owner[t]
            p = ids_s[8, o]
            ids_s[8, o] = p + 1
            ids_s[o >> 3, ((o & 7) << 4) + p] = row[t]
            base = step * 32 + k
            block = o * (2 * BLOCK) + p
            send[pl.ds(block, 2, stride=SLOTS), :] = x[pl.ds(base, 2, stride=8), :]
            send[pl.ds(block + BLOCK, 2, stride=SLOTS), :] = x[pl.ds(base + 16, 2, stride=8), :]
        return 0

    lax.fori_loop(0, TOKENS // 8, tokens, 0)
    copy = pltpu.make_async_copy(ids_s, ids_v, sem)
    copy.start()
    copy.wait()
    ids = ids_v[0:8, :].astype(jnp.float32)
    mine = lax.rem(lax.axis_index("dp") * 2 + lax.axis_index("rep"), 8)
    lane = lax.broadcasted_iota(jnp.int32, (8, 128), 1)
    for b in range(8):
        turned = pltpu.roll(ids, lax.rem((mine - b + 8) * SLOTS, 128), 1)
        line = jnp.where((lane >> 4) == mine, turned, 0.0)
        for h in range(2):
            send[pl.ds((2 * b + h) * BLOCK + 2 * SLOTS, 8, stride=16 * BLOCK), :] = line


def pack(owner, row, x):
    return pl.pallas_call(
        pack_kernel,
        out_shape=jax.ShapeDtypeStruct((DEVICES * BLOCK, 128), jnp.float32),
        in_specs=[
            pl.BlockSpec(memory_space=SMEM),
            pl.BlockSpec(memory_space=SMEM),
            pl.BlockSpec(memory_space=VMEM),
        ],
        out_specs=pl.BlockSpec(memory_space=VMEM),
        scratch_shapes=[
            pltpu.VMEM((16, 128), jnp.int32),
            pltpu.SMEM((16, 128), jnp.int32),
            pltpu.SemaphoreType.DMA,
        ],
        compiler_params=pltpu.CompilerParams(vmem_limit_bytes=8 * 2**20),
        name="pack",
    )(owner, row, x)


def sum_kernel(recv, half, squares, ids_v, ids_s, sem, *sums):
    for g in range(16):
        lines = recv[pl.ds(g * 8 * BLOCK + 2 * SLOTS, 8, stride=BLOCK), :]
        ids_v[g : g + 1, :] = jnp.sum(lines, axis=0, keepdims=True).astype(jnp.int32)
    copy = pltpu.make_async_copy(ids_v, ids_s, sem)
    copy.start()

    def clear(i, _):
        for total in sums:
            for k in range(8):
                total[pl.ds(i * 64 + k * 8, 8), :] = jnp.zeros((8, 128), jnp.float32)
        return 0

    lax.fori_loop(0, 2 * PITCH // 64, clear, 0)
    for total in sums:
        for k in range(2 * PITCH // 64 * 64, 2 * PITCH, 8):
            total[k : k + 8, :] = jnp.zeros((8, 128), jnp.float32)
    copy.wait()
    groups = 16 // CHAINS

    def add(i, _):
        g, s = i // 8, lax.rem(i, 8)
        for p in range(SLOTS):
            for c, total in enumerate(sums):
                r = ids_s[g + c * groups, s * SLOTS + p]
                line = ((g + c * groups) * 8 + s) * BLOCK + p
                spot = pl.ds(r, 2, stride=PITCH)
                total[spot, :] = total[spot, :] + recv[pl.ds(line, 2, stride=SLOTS), :]
        return 0

    lax.fori_loop(0, groups * 8, add, 0)

    def fold(i, squared):
        squared = list(squared)
        for k in range(4):
            for j in range(2):
                at = pl.multiple_of(j * PITCH + i * 32 + k * 8, 8)
                parts = [total[pl.ds(at, 8), :] for total in sums]
                while len(parts) > 1:
                    parts = [a + b for a, b in zip(parts[::2], parts[1::2])]
                half[pl.ds(pl.multiple_of(i * 32 + k * 8, 8), 8), j * 128 : (j + 1) * 128] = parts[0]
                squared[k] = squared[k] + parts[0] * parts[0]
        return tuple(squared)

    zero = jnp.zeros((8, 128), jnp.float32)
    a, b, c, d = lax.fori_loop(0, ROWS // 32, fold, (zero,) * 4)
    squares[...] = jnp.broadcast_to(jnp.sum((a + b) + (c + d), axis=0, keepdims=True), squares.shape)


def sum_rows(recv):
    return pl.pallas_call(
        sum_kernel,
        out_shape=(
            jax.ShapeDtypeStruct((ROWS, 256), jnp.float32),
            jax.ShapeDtypeStruct((DEVICES, 128), jnp.float32),
        ),
        in_specs=[pl.BlockSpec(memory_space=VMEM)],
        out_specs=(pl.BlockSpec(memory_space=VMEM), pl.BlockSpec(memory_space=VMEM)),
        scratch_shapes=[
            pltpu.VMEM((16, 128), jnp.int32),
            pltpu.SMEM((16, 128), jnp.int32),
            pltpu.SemaphoreType.DMA,
        ]
        + [pltpu.VMEM((2 * PITCH, 128), jnp.float32)] * CHAINS,
        compiler_params=pltpu.CompilerParams(vmem_limit_bytes=18 * 2**20),
        name="sum_rows",
    )(recv)


def update_kernel(part, own, other, table, moment, second, *rest):
    outs, bufs, sems = rest[0:3], rest[3:6], rest[6]
    total = jnp.sum(part[...], keepdims=True)
    limit = 0.5 * float(VOCAB * LW) ** 0.5
    clip = jnp.minimum(1.0, limit / (jnp.sqrt(total) + 1e-06))
    scale = jnp.broadcast_to(clip, (8, 128))
    first_fix = 1.0 - 0.9**ADAM_STEP
    second_fix = 1.0 - 0.999**ADAM_STEP
    rep = lax.axis_index("rep")
    new_table, new_moment, new_second = bufs

    def tile(i, _):
        for k in range(2):
            rows = pl.ds(pl.multiple_of(i * 16 + k * 8, 8), 8)
            for h, source in enumerate((own, other)):
                start = jnp.where(rep == 0, h, 1 - h) * 256
                for j in range(2):
                    cols = pl.ds(pl.multiple_of(start + j * 128, 128), 128)
                    g = scale * source[rows, j * 128 : (j + 1) * 128]
                    nm = 0.9 * moment[rows, cols] + 0.1 * g
                    nv = 0.999 * second[rows, cols] + 0.001 * g * g
                    root = jnp.sqrt(nv * (1.0 / second_fix)) + 1e-08
                    t = table[rows, cols]
                    new_moment[rows, cols] = nm
                    new_second[rows, cols] = nv
                    new_table[rows, cols] = t - 0.01 * ((nm * (1.0 / first_fix)) / root + 0.01 * t)
        return 0

    def copies(c):
        rows = pl.ds(pl.multiple_of(c * CHUNK, CHUNK), CHUNK)
        return [
            pltpu.make_async_copy(buf.at[rows], out.at[rows], sems.at[n, c])
            for n, (buf, out) in enumerate(zip(bufs, outs))
        ]

    steps = CHUNK // 16
    for c in range(ROWS // CHUNK):
        lax.fori_loop(c * steps, (c + 1) * steps, tile, 0)
        for copy in copies(c):
            copy.start()
    for c in range(ROWS // CHUNK):
        for copy in copies(c):
            copy.wait()


def update(part, own, other, table, moment, second):
    shape = jax.ShapeDtypeStruct((ROWS, LW), jnp.float32)
    return pl.pallas_call(
        update_kernel,
        out_shape=(shape,) * 3,
        in_specs=[pl.BlockSpec(memory_space=VMEM)] * 6,
        out_specs=(pl.BlockSpec(memory_space=pl.ANY),) * 3,
        scratch_shapes=[pltpu.VMEM((ROWS, LW), jnp.float32)] * 3
        + [pltpu.SemaphoreType.DMA((3, ROWS // CHUNK))],
        compiler_params=pltpu.CompilerParams(vmem_limit_bytes=34 * 2**20),
        name="update",
    )(part, own, other, table, moment, second)


def local(row_grads, token_owner, token_row, table, moment, second):
    x = row_grads.reshape(64, 8, 4, 128).transpose(0, 2, 1, 3).reshape(4 * TOKENS, 128)
    send = pack(token_owner[:, 0], token_row, x)
    recv = lax.all_to_all(send.reshape(DEVICES, 1, BLOCK * 128), AXES, 0, 0, tiled=True)
    half, squares = sum_rows(recv.reshape(DEVICES * BLOCK, 128))
    part = lax.all_to_all(squares.reshape(DEVICES, 1, 128), AXES, 0, 0, tiled=True)
    other = lax.ppermute(half, "rep", [(0, 1), (1, 0)])
    return update(part.reshape(DEVICES, 128), half, other, table, moment, second)


def solution(mesh):
    return jax.shard_map(
        local,
        mesh=mesh,
        in_specs=(
            P(("dp", "rep"), None),
            P(("dp", "rep"), None),
            P(("dp", "rep")),
            P("dp", None),
            P("dp", None),
            P("dp", None),
        ),
        out_specs=(P("dp", None), P("dp", None), P("dp", None)),
        check_vma=False,
    )
```

```python
import jax
import jax.numpy as jnp
from jax import lax
from jax.experimental import pallas as pl
from jax.experimental.pallas import tpu as pltpu
from jax.sharding import PartitionSpec as P

VOCAB = 131072
ADAM_STEP = 100
LW = 512
OWNERS = 64
SLOTS = 16
TOKENS = 512
ROWS = 2048
DEVICES = 128
BLOCK = 2 * SLOTS + 1
PITCH = 2064
CHAINS = 8
CHUNK = 16
AXES = ("dp", "rep")
VMEM = pltpu.MemorySpace.VMEM
SMEM = pltpu.MemorySpace.SMEM
HBM = pltpu.MemorySpace.HBM


def pack_kernel(owner, row, x, send, owner_v, row_v, x_v, dest_v, dest_s, sems):
    loads = [
        pltpu.make_async_copy(a, b, sems.at[n])
        for n, (a, b) in enumerate(((owner, owner_v), (row, row_v), (x, x_v)))
    ]
    for load in loads:
        load.start()
    early = lax.broadcasted_iota(jnp.int32, (128, 128), 0)
    late = lax.broadcasted_iota(jnp.int32, (128, 128), 1)
    before = jnp.where(early < late, 1.0, 0.0).astype(jnp.bfloat16)
    ones = jnp.ones((128, 128), jnp.bfloat16)
    who = lax.broadcasted_iota(jnp.int32, (OWNERS, 128), 0)
    base = (who * (2 * BLOCK)).astype(jnp.float32)
    mine = lax.rem(lax.axis_index("dp") * 2 + lax.axis_index("rep"), 8)
    loads[0].wait()
    masks = [who == owner_v[i : i + 1, :] for i in range(4)]
    hots = [jnp.where(mask, 1.0, 0.0).astype(jnp.bfloat16) for mask in masks]
    hot = jnp.concatenate(hots, axis=0)
    inside = jnp.dot(hot, before, preferred_element_type=jnp.float32)
    counts = jnp.dot(hot, ones, preferred_element_type=jnp.float32)
    seen = jnp.zeros((OWNERS, 128), jnp.float32)
    positions = []
    for i in range(4):
        part = slice(i * OWNERS, (i + 1) * OWNERS)
        at = jnp.where(masks[i], inside[part] + seen, 0.0)
        positions.append(jnp.sum(at, axis=0, keepdims=True))
        start = jnp.sum(jnp.where(masks[i], base, 0.0), axis=0, keepdims=True)
        dest_v[i : i + 1, :] = (start + positions[i]).astype(jnp.int32)
        seen = seen + counts[part]
    move = pltpu.make_async_copy(dest_v, dest_s, sems.at[3])
    move.start()
    loads[1].wait()
    lines = early - mine * SLOTS
    ids = jnp.zeros((OWNERS, 256), jnp.float32)
    for i in range(4):
        left = ROWS - row_v[i : i + 1, :]
        here = lines == positions[i].astype(jnp.int32)
        high = jnp.where(here, (left >> 4).astype(jnp.float32), 0.0)
        low = jnp.where(here, (left & 15).astype(jnp.float32), 0.0)
        both = jnp.concatenate([high, low], axis=0).astype(jnp.bfloat16)
        ids = ids + lax.dot_general(
            hots[i], both, (((1,), (1,)), ((), ())), preferred_element_type=jnp.float32
        )
    ids = ROWS - (16.0 * ids[:, :128] + ids[:, 128:])
    lane = lax.broadcasted_iota(jnp.int32, (OWNERS, 128), 1)
    ids = jnp.where((lane >> 4) == mine, ids, 0.0)
    for a in range(OWNERS // 8):
        for h in range(2):
            spot = (16 * a + h) * BLOCK + 2 * SLOTS
            send[pl.ds(spot, 8, stride=2 * BLOCK), :] = ids[8 * a : 8 * a + 8]
    loads[2].wait()
    move.wait()

    def tokens(step, _):
        rows = x_v.at[pl.ds(pl.multiple_of(step * 512, 512), 512)]
        for k in range(128):
            block = dest_s[step, k]
            base = k // 8 * 32 + k % 8
            send[pl.ds(block, 2, stride=SLOTS), :] = rows[pl.ds(base, 2, stride=8), :]
            send[pl.ds(block + BLOCK, 2, stride=SLOTS), :] = rows[pl.ds(base + 16, 2, stride=8), :]
        return 0

    lax.fori_loop(0, TOKENS // 128, tokens, 0)


def pack(owner, row, x):
    return pl.pallas_call(
        pack_kernel,
        out_shape=jax.ShapeDtypeStruct((DEVICES * BLOCK, 128), jnp.float32),
        in_specs=[pl.BlockSpec(memory_space=HBM)] * 3,
        out_specs=pl.BlockSpec(memory_space=VMEM),
        scratch_shapes=[
            pltpu.VMEM((4, 128), jnp.int32),
            pltpu.VMEM((4, 128), jnp.int32),
            pltpu.VMEM((4 * TOKENS, 128), jnp.float32),
            pltpu.VMEM((4, 128), jnp.int32),
            pltpu.SMEM((4, 128), jnp.int32),
            pltpu.SemaphoreType.DMA((4,)),
        ],
        compiler_params=pltpu.CompilerParams(vmem_limit_bytes=5 * 2**20),
        name="pack",
    )(*(pltpu.with_memory_space_constraint(a, HBM) for a in (owner, row, x)))


def sum_kernel(recv, second, half, squares, second_v, ids_v, ids_s, sem, second_sem, *sums):
    fetch = pltpu.make_async_copy(second, second_v, second_sem)
    fetch.start()
    for g in range(16):
        lines = recv[pl.ds(g * 8 * BLOCK + 2 * SLOTS, 8, stride=BLOCK), :]
        ids_v[g : g + 1, :] = jnp.sum(lines, axis=0, keepdims=True).astype(jnp.int32)
    copy = pltpu.make_async_copy(ids_v, ids_s, sem)
    copy.start()

    def clear(i, _):
        for total in sums:
            for k in range(8):
                total[pl.ds(i * 64 + k * 8, 8), :] = jnp.zeros((8, 128), jnp.float32)
        return 0

    lax.fori_loop(0, 2 * PITCH // 64, clear, 0)
    for total in sums:
        for k in range(2 * PITCH // 64 * 64, 2 * PITCH, 8):
            total[k : k + 8, :] = jnp.zeros((8, 128), jnp.float32)
    copy.wait()
    groups = 16 // CHAINS

    def add(g, _):
        lines = [
            recv.at[pl.ds(pl.multiple_of((c * groups + g) * 8 * BLOCK, 8), 8 * BLOCK)]
            for c in range(CHAINS)
        ]
        for at in range(8 * SLOTS):
            line = at // SLOTS * BLOCK + at % SLOTS
            for c, total in enumerate(sums):
                spot = pl.ds(ids_s[c * groups + g, at], 2, stride=PITCH)
                total[spot, :] = total[spot, :] + lines[c][pl.ds(line, 2, stride=SLOTS), :]
        return 0

    lax.fori_loop(0, groups, add, 0)

    def fold(i, squared):
        squared = list(squared)
        for k in range(8):
            for j in range(2):
                at = pl.multiple_of(j * PITCH + i * 64 + k * 8, 8)
                parts = [total[pl.ds(at, 8), :] for total in sums]
                while len(parts) > 1:
                    parts = [a + b for a, b in zip(parts[::2], parts[1::2])]
                half[i * 8 + k, j] = parts[0]
                squared[k % 4] = squared[k % 4] + parts[0] * parts[0]
        return tuple(squared)

    zero = jnp.zeros((8, 128), jnp.float32)
    a, b, c, d = lax.fori_loop(0, ROWS // 64, fold, (zero,) * 4)
    squares[...] = jnp.broadcast_to(jnp.sum((a + b) + (c + d), axis=0, keepdims=True), squares.shape)
    fetch.wait()


def sum_rows(recv, second):
    return pl.pallas_call(
        sum_kernel,
        out_shape=(
            jax.ShapeDtypeStruct((ROWS // 8, 2, 8, 128), jnp.float32),
            jax.ShapeDtypeStruct((DEVICES, 128), jnp.float32),
            jax.ShapeDtypeStruct((ROWS // 8, 4, 8, 128), jnp.float32),
        ),
        in_specs=[pl.BlockSpec(memory_space=VMEM), pl.BlockSpec(memory_space=HBM)],
        out_specs=(pl.BlockSpec(memory_space=VMEM),) * 3,
        scratch_shapes=[
            pltpu.VMEM((16, 128), jnp.int32),
            pltpu.SMEM((16, 128), jnp.int32),
            pltpu.SemaphoreType.DMA,
            pltpu.SemaphoreType.DMA,
        ]
        + [pltpu.VMEM((2 * PITCH, 128), jnp.float32)] * CHAINS,
        compiler_params=pltpu.CompilerParams(vmem_limit_bytes=22 * 2**20),
        name="sum_rows",
    )(recv, pltpu.with_memory_space_constraint(second, HBM))


def update_kernel(part, own, other, table, moment, second, *rest):
    outs, bufs, sems = rest[0:3], rest[3:6], rest[6]
    total = jnp.sum(part[...], keepdims=True)
    limit = 0.5 * float(VOCAB * LW) ** 0.5
    clip = jnp.minimum(1.0, limit / (jnp.sqrt(total) + 1e-06))
    first_fix = 1.0 - 0.9**ADAM_STEP
    second_fix = 1.0 - 0.999**ADAM_STEP
    to_moment = jnp.broadcast_to(0.1 * clip, (8, 128))
    to_second = jnp.broadcast_to(0.001 * clip * clip, (8, 128))
    rep = lax.axis_index("rep")

    def tile(i, _):
        rows = pl.ds(i * 4, 4)
        for h, source in enumerate((own, other)):
            cols = pl.ds(jnp.where(rep == 0, h, 1 - h) * 2, 2)
            ins = [ref.at[rows, cols] for ref in (table, moment, second)]
            to = [ref.at[rows, cols] for ref in bufs]
            grads = source.at[rows]
            for k in range(4):
                for j in range(2):
                    g = grads[k, j]
                    nm = 0.9 * ins[1][k, j] + to_moment * g
                    nv = 0.999 * ins[2][k, j] + to_second * (g * g)
                    root = (nv * lax.rsqrt(nv)) * (1.0 / second_fix) ** 0.5 + 1e-08
                    to[1][k, j] = nm
                    to[2][k, j] = nv
                    step = (nm * (0.01 / first_fix)) / root
                    to[0][k, j] = (1.0 - 0.0001) * ins[0][k, j] - step
        return 0

    def copies(c):
        rows = pl.ds(c * CHUNK, CHUNK)
        return [
            pltpu.make_async_copy(buf.at[rows], out.at[rows], sems.at[n, c])
            for n, (buf, out) in enumerate(zip(bufs, outs))
        ]

    steps = CHUNK // 4
    for c in range(ROWS // 8 // CHUNK):
        lax.fori_loop(c * steps, (c + 1) * steps, tile, 0)
        for copy in copies(c):
            copy.start()
    for c in range(ROWS // 8 // CHUNK):
        for copy in copies(c):
            copy.wait()


def update(part, own, other, table, moment, second):
    shape = jax.ShapeDtypeStruct((ROWS // 8, 4, 8, 128), jnp.float32)
    return pl.pallas_call(
        update_kernel,
        out_shape=(shape,) * 3,
        in_specs=[pl.BlockSpec(memory_space=VMEM)] * 6,
        out_specs=(pl.BlockSpec(memory_space=pl.ANY),) * 3,
        scratch_shapes=[pltpu.VMEM((ROWS // 8, 4, 8, 128), jnp.float32)] * 3
        + [pltpu.SemaphoreType.DMA((3, ROWS // 8 // CHUNK))],
        compiler_params=pltpu.CompilerParams(vmem_limit_bytes=30 * 2**20),
        name="update",
    )(part, own, other, table, moment, second)


def tiles(array):
    rows, cols = array.shape
    return array.reshape(rows // 8, 8, cols // 128, 128).transpose(0, 2, 1, 3)


def local(row_grads, token_owner, token_row, table, moment, second):
    x = tiles(row_grads).reshape(4 * TOKENS, 128)
    send = pack(token_owner.reshape(4, 128), token_row.reshape(4, 128), x)
    recv = lax.all_to_all(send.reshape(DEVICES, 1, BLOCK * 128), AXES, 0, 0, tiled=True)
    half, squares, second = sum_rows(recv.reshape(DEVICES * BLOCK, 128), tiles(second))
    part = lax.all_to_all(squares.reshape(DEVICES, 1, 128), AXES, 0, 0, tiled=True)
    other = lax.ppermute(half, "rep", [(0, 1), (1, 0)])
    outs = update(part.reshape(DEVICES, 128), half, other, tiles(table), tiles(moment), second)
    return tuple(out.transpose(0, 2, 1, 3).reshape(ROWS, LW) for out in outs)


def solution(mesh):
    return jax.shard_map(
        local,
        mesh=mesh,
        in_specs=(
            P(("dp", "rep"), None),
            P(("dp", "rep"), None),
            P(("dp", "rep")),
            P("dp", None),
            P("dp", None),
            P("dp", None),
        ),
        out_specs=(P("dp", None), P("dp", None), P("dp", None)),
        check_vma=False,
    )
```

```python
import jax
import jax.numpy as jnp
from jax import lax
from jax.experimental import pallas as pl
from jax.experimental.pallas import tpu as pltpu
from jax.sharding import PartitionSpec as P

VOCAB = 131072
ADAM_STEP = 100
LW = 512
OWNERS = 64
SLOTS = 16
TOKENS = 512
ROWS = 2048
DEVICES = 128
BLOCK = 2 * SLOTS + 1
PITCH = 2064
CHAINS = 6
CHUNKS = (16, 24, 32, 48, 64, 72)
AXES = ("dp", "rep")
VMEM = pltpu.MemorySpace.VMEM
SMEM = pltpu.MemorySpace.SMEM
HBM = pltpu.MemorySpace.HBM


def pack_kernel(owner, row, x, send, *refs):
    sums = refs[:CHAINS]
    owner_v, row_v, x_v, dest_v, dest_s, sems = refs[CHAINS:]
    loads = [
        pltpu.make_async_copy(a, b, sems.at[n])
        for n, (a, b) in enumerate(((owner, owner_v), (row, row_v), (x, x_v)))
    ]
    for load in loads:
        load.start()
    early = lax.broadcasted_iota(jnp.int32, (128, 128), 0)
    late = lax.broadcasted_iota(jnp.int32, (128, 128), 1)
    before = jnp.where(early < late, 1.0, 0.0).astype(jnp.bfloat16)
    ones = jnp.ones((128, 128), jnp.bfloat16)
    who = lax.broadcasted_iota(jnp.int32, (OWNERS, 128), 0)
    base = (who * (2 * BLOCK)).astype(jnp.float32)
    mine = lax.rem(lax.axis_index("dp") * 2 + lax.axis_index("rep"), 8)

    def clear(i, _):
        for total in sums:
            for k in range(4):
                total[pl.ds(i * 32 + k * 8, 8), :] = jnp.zeros((8, 128), jnp.float32)
        return 0

    lax.fori_loop(0, 2 * PITCH // 64, clear, 0)
    loads[0].wait()
    masks = [who == owner_v[i : i + 1, :] for i in range(4)]
    hots = [jnp.where(mask, 1.0, 0.0).astype(jnp.bfloat16) for mask in masks]
    hot = jnp.concatenate(hots, axis=0)
    inside = jnp.dot(hot, before, preferred_element_type=jnp.float32)
    counts = jnp.dot(hot, ones, preferred_element_type=jnp.float32)
    seen = jnp.zeros((OWNERS, 128), jnp.float32)
    positions = []
    for i in range(4):
        part = slice(i * OWNERS, (i + 1) * OWNERS)
        at = jnp.where(masks[i], inside[part] + seen, 0.0)
        positions.append(jnp.sum(at, axis=0, keepdims=True))
        start = jnp.sum(jnp.where(masks[i], base, 0.0), axis=0, keepdims=True)
        dest_v[i : i + 1, :] = (start + positions[i]).astype(jnp.int32)
        seen = seen + counts[part]
    move = pltpu.make_async_copy(dest_v, dest_s, sems.at[3])
    move.start()
    loads[1].wait()
    lines = early - mine * SLOTS
    ids = jnp.zeros((OWNERS, 256), jnp.float32)
    for i in range(4):
        left = ROWS - row_v[i : i + 1, :]
        here = lines == positions[i].astype(jnp.int32)
        high = jnp.where(here, (left >> 4).astype(jnp.float32), 0.0)
        low = jnp.where(here, (left & 15).astype(jnp.float32), 0.0)
        both = jnp.concatenate([high, low], axis=0).astype(jnp.bfloat16)
        ids = ids + lax.dot_general(
            hots[i], both, (((1,), (1,)), ((), ())), preferred_element_type=jnp.float32
        )
    ids = ROWS - (16.0 * ids[:, :128] + ids[:, 128:])
    lane = lax.broadcasted_iota(jnp.int32, (OWNERS, 128), 1)
    ids = jnp.where(ids == ROWS, (ROWS + (lane & 15)).astype(jnp.float32), ids)
    ids = jnp.where((lane >> 4) == mine, ids, 0.0)
    for a in range(OWNERS // 8):
        for h in range(2):
            spot = (16 * a + h) * BLOCK + 2 * SLOTS
            send[pl.ds(spot, 8, stride=2 * BLOCK), :] = ids[8 * a : 8 * a + 8]
    lax.fori_loop(2 * PITCH // 64, 2 * PITCH // 32, clear, 0)
    loads[2].wait()
    move.wait()

    def tokens(step, _):
        rows = x_v.at[pl.ds(pl.multiple_of(step * 512, 512), 512)]
        for k in range(128):
            block = dest_s[step, k]
            base = k // 8 * 32 + k % 8
            send[pl.ds(block, 2, stride=SLOTS), :] = rows[pl.ds(base, 2, stride=8), :]
            send[pl.ds(block + BLOCK, 2, stride=SLOTS), :] = rows[pl.ds(base + 16, 2, stride=8), :]
        return 0

    lax.fori_loop(0, TOKENS // 128, tokens, 0)


def pack(owner, row, x):
    return pl.pallas_call(
        pack_kernel,
        out_shape=(jax.ShapeDtypeStruct((DEVICES * BLOCK, 128), jnp.float32),)
        + (jax.ShapeDtypeStruct((2 * PITCH, 128), jnp.float32),) * CHAINS,
        in_specs=[pl.BlockSpec(memory_space=HBM)] * 3,
        out_specs=(pl.BlockSpec(memory_space=VMEM),) * (1 + CHAINS),
        scratch_shapes=[
            pltpu.VMEM((4, 128), jnp.int32),
            pltpu.VMEM((4, 128), jnp.int32),
            pltpu.VMEM((4 * TOKENS, 128), jnp.float32),
            pltpu.VMEM((4, 128), jnp.int32),
            pltpu.SMEM((4, 128), jnp.int32),
            pltpu.SemaphoreType.DMA((4,)),
        ],
        compiler_params=pltpu.CompilerParams(vmem_limit_bytes=20 * 2**20),
        name="pack",
    )(*(pltpu.with_memory_space_constraint(a, HBM) for a in (owner, row, x)))


def sum_kernel(recv, second, *refs):
    half, squares, second_v = refs[CHAINS : CHAINS + 3]
    sums = refs[CHAINS + 3 : 2 * CHAINS + 3]
    ids_v, ids_s, id_sems, sem = refs[2 * CHAINS + 3 :]
    fetch = pltpu.make_async_copy(second, second_v, sem)
    def move(q):
        part = pl.ds(pl.multiple_of(q * 8, 8), 8)
        return pltpu.make_async_copy(ids_v.at[part], ids_s.at[part], id_sems.at[q])

    for g in range(16):
        lines = recv[pl.ds(g * 8 * BLOCK + 2 * SLOTS, 8, stride=BLOCK), :]
        at = g // 4 * 8 + g % 4
        ids_v[at : at + 1, :] = jnp.sum(lines, axis=0, keepdims=True).astype(jnp.int32)
        if g % 4 == 3:
            move(g // 4).start()

    fetch.start()

    def add(g, _):
        q, k = g >> 2, g & 3

        @pl.when(k == 0)
        def _():
            move(q).wait()

        lines = recv.at[pl.ds(pl.multiple_of(g * 8 * BLOCK, 8), 8 * BLOCK)]
        for at in range(8 * SLOTS):
            total = sums[at % CHAINS]
            line = at // SLOTS * BLOCK + at % SLOTS
            spot = pl.ds(ids_s[q * 8 + k, at], 2, stride=PITCH)
            total[spot, :] = total[spot, :] + lines[pl.ds(line, 2, stride=SLOTS), :]
        return 0

    lax.fori_loop(0, 16, add, 0)

    def fold(i, squared):
        squared = list(squared)
        for k in range(8):
            for j in range(2):
                at = pl.multiple_of(j * PITCH + i * 64 + k * 8, 8)
                parts = [total[pl.ds(at, 8), :] for total in sums]
                while len(parts) > 1:
                    parts = [sum(parts[k : k + 2]) for k in range(0, len(parts), 2)]
                half[i * 8 + k, j] = parts[0]
                squared[k % 4] = squared[k % 4] + parts[0] * parts[0]
        return tuple(squared)

    zero = jnp.zeros((8, 128), jnp.float32)
    a, b, c, d = lax.fori_loop(0, ROWS // 64, fold, (zero,) * 4)
    squares[...] = jnp.broadcast_to(jnp.sum((a + b) + (c + d), axis=0, keepdims=True), squares.shape)
    fetch.wait()


def sum_rows(recv, second, sums):
    total = jax.ShapeDtypeStruct((2 * PITCH, 128), jnp.float32)
    return pl.pallas_call(
        sum_kernel,
        out_shape=(
            jax.ShapeDtypeStruct((ROWS // 8, 2, 8, 128), jnp.float32),
            jax.ShapeDtypeStruct((DEVICES, 128), jnp.float32),
            jax.ShapeDtypeStruct((ROWS // 8, 4, 8, 128), jnp.float32),
        )
        + (total,) * CHAINS,
        in_specs=[pl.BlockSpec(memory_space=VMEM), pl.BlockSpec(memory_space=HBM)]
        + [pl.BlockSpec(memory_space=VMEM)] * CHAINS,
        out_specs=(pl.BlockSpec(memory_space=VMEM),) * (3 + CHAINS),
        scratch_shapes=[
            pltpu.VMEM((32, 128), jnp.int32),
            pltpu.SMEM((32, 128), jnp.int32),
            pltpu.SemaphoreType.DMA((4,)),
            pltpu.SemaphoreType.DMA,
        ],
        input_output_aliases={2 + c: 3 + c for c in range(CHAINS)},
        compiler_params=pltpu.CompilerParams(vmem_limit_bytes=22 * 2**20),
        name="sum_rows",
    )(recv, pltpu.with_memory_space_constraint(second, HBM), *sums)


def update_kernel(part, own, other, table, moment, second, *rest):
    outs, bufs, sems = rest[0:3], rest[3:6], rest[6]
    total = jnp.sum(part[...], keepdims=True)
    limit = 0.5 * float(VOCAB * LW) ** 0.5
    clip = jnp.minimum(1.0, limit / (jnp.sqrt(total) + 1e-06))
    first_fix = 1.0 - 0.9**ADAM_STEP
    second_fix = 1.0 - 0.999**ADAM_STEP
    to_moment = jnp.broadcast_to(0.1 * clip, (8, 128))
    to_second = jnp.broadcast_to(0.001 * clip * clip, (8, 128))
    rep = lax.axis_index("rep")

    def tile(i, _):
        rows = pl.ds(i * 4, 4)
        for h, source in enumerate((own, other)):
            cols = pl.ds(jnp.where(rep == 0, h, 1 - h) * 2, 2)
            ins = [ref.at[rows, cols] for ref in (table, moment, second)]
            to = [ref.at[rows, cols] for ref in bufs]
            grads = source.at[rows]
            for k in range(4):
                for j in range(2):
                    g = grads[k, j]
                    nm = 0.9 * ins[1][k, j] + to_moment * g
                    nv = 0.999 * ins[2][k, j] + to_second * (g * g)
                    root = (nv * lax.rsqrt(nv)) * (1.0 / second_fix) ** 0.5 + 1e-08
                    to[1][k, j] = nm
                    to[2][k, j] = nv
                    step = (nm * (0.01 / first_fix)) / root
                    to[0][k, j] = (1.0 - 0.0001) * ins[0][k, j] - step
        return 0

    def copies(c, first):
        rows = pl.ds(first, CHUNKS[c])
        return [
            pltpu.make_async_copy(buf.at[rows], out.at[rows], sems.at[n, c])
            for n, (buf, out) in enumerate(zip(bufs, outs))
        ]

    first = 0
    started = []
    for c, count in enumerate(CHUNKS):
        lax.fori_loop(first // 4, (first + count) // 4, tile, 0)
        chunk = copies(c, first)
        for copy in chunk:
            copy.start()
        started += chunk
        first += count
    for copy in started:
        copy.wait()


def update(part, own, other, table, moment, second):
    shape = jax.ShapeDtypeStruct((ROWS // 8, 4, 8, 128), jnp.float32)
    return pl.pallas_call(
        update_kernel,
        out_shape=(shape,) * 3,
        in_specs=[pl.BlockSpec(memory_space=VMEM)] * 6,
        out_specs=(pl.BlockSpec(memory_space=pl.ANY),) * 3,
        scratch_shapes=[pltpu.VMEM((ROWS // 8, 4, 8, 128), jnp.float32)] * 3
        + [pltpu.SemaphoreType.DMA((3, len(CHUNKS)))],
        compiler_params=pltpu.CompilerParams(vmem_limit_bytes=30 * 2**20),
        name="update",
    )(part, own, other, table, moment, second)


def tiles(array):
    rows, cols = array.shape
    return array.reshape(rows // 8, 8, cols // 128, 128).transpose(0, 2, 1, 3)


def local(row_grads, token_owner, token_row, table, moment, second):
    x = tiles(row_grads).reshape(4 * TOKENS, 128)
    send, *sums = pack(token_owner.reshape(4, 128), token_row.reshape(4, 128), x)
    recv = lax.all_to_all(send.reshape(DEVICES, 1, BLOCK * 128), AXES, 0, 0, tiled=True)
    lines = recv.reshape(DEVICES * BLOCK, 128)
    half, squares, second = sum_rows(lines, tiles(second), sums)[:3]
    part = lax.all_to_all(squares.reshape(DEVICES, 1, 128), AXES, 0, 0, tiled=True)
    other = lax.ppermute(half, "rep", [(0, 1), (1, 0)])
    outs = update(part.reshape(DEVICES, 128), half, other, tiles(table), tiles(moment), second)
    return tuple(out.transpose(0, 2, 1, 3).reshape(ROWS, LW) for out in outs)


def solution(mesh):
    return jax.shard_map(
        local,
        mesh=mesh,
        in_specs=(
            P(("dp", "rep"), None),
            P(("dp", "rep"), None),
            P(("dp", "rep")),
            P("dp", None),
            P("dp", None),
            P("dp", None),
        ),
        out_specs=(P("dp", None), P("dp", None), P("dp", None)),
        check_vma=False,
    )
```

```python
import jax
import jax.numpy as jnp
from jax import lax
from jax.experimental import pallas as pl
from jax.experimental.pallas import tpu as pltpu
from jax.sharding import PartitionSpec as P

VOCAB = 131072
ADAM_STEP = 100
LW = 512
OWNERS = 64
SLOTS = 16
TOKENS = 512
ROWS = 2048
DEVICES = 128
BLOCK = 2 * SLOTS + 1
PITCH = 2064
CHAINS = 6
CHUNKS = (8, 16, 24, 36, 52, 64, 56)
AXES = ("dp", "rep")
VMEM = pltpu.MemorySpace.VMEM
SMEM = pltpu.MemorySpace.SMEM
HBM = pltpu.MemorySpace.HBM


def pack_kernel(owner, row, x, send, *refs):
    sums = refs[:CHAINS]
    owner_v, row_v, x_v, dest_v, dest_s, sems = refs[CHAINS:]
    loads = [
        pltpu.make_async_copy(a, b, sems.at[n])
        for n, (a, b) in enumerate(((owner, owner_v), (row, row_v), (x, x_v)))
    ]
    for load in loads:
        load.start()
    early = lax.broadcasted_iota(jnp.int32, (128, 128), 0)
    late = lax.broadcasted_iota(jnp.int32, (128, 128), 1)
    before = jnp.where(early < late, 1.0, 0.0).astype(jnp.bfloat16)
    ones = jnp.ones((128, 128), jnp.bfloat16)
    who = lax.broadcasted_iota(jnp.int32, (OWNERS, 128), 0)
    base = (who * (2 * BLOCK)).astype(jnp.float32)
    mine = lax.rem(lax.axis_index("dp") * 2 + lax.axis_index("rep"), 8)

    def clear(i, _):
        for total in sums:
            for k in range(4):
                total[pl.ds(i * 32 + k * 8, 8), :] = jnp.zeros((8, 128), jnp.float32)
        return 0

    lax.fori_loop(0, 2 * PITCH // 64, clear, 0)
    loads[0].wait()
    masks = [who == owner_v[i : i + 1, :] for i in range(4)]
    hots = [jnp.where(mask, 1.0, 0.0).astype(jnp.bfloat16) for mask in masks]
    hot = jnp.concatenate(hots, axis=0)
    inside = jnp.dot(hot, before, preferred_element_type=jnp.float32)
    counts = jnp.dot(hot, ones, preferred_element_type=jnp.float32)
    seen = jnp.zeros((OWNERS, 128), jnp.float32)
    positions = []
    for i in range(4):
        part = slice(i * OWNERS, (i + 1) * OWNERS)
        at = jnp.where(masks[i], inside[part] + seen, 0.0)
        positions.append(jnp.sum(at, axis=0, keepdims=True))
        start = jnp.sum(jnp.where(masks[i], base, 0.0), axis=0, keepdims=True)
        dest_v[i : i + 1, :] = (start + positions[i]).astype(jnp.int32)
        seen = seen + counts[part]
    move = pltpu.make_async_copy(dest_v, dest_s, sems.at[3])
    move.start()
    loads[1].wait()
    lines = early - mine * SLOTS
    ids = jnp.zeros((OWNERS, 256), jnp.float32)
    for i in range(4):
        left = ROWS - row_v[i : i + 1, :]
        here = lines == positions[i].astype(jnp.int32)
        high = jnp.where(here, (left >> 4).astype(jnp.float32), 0.0)
        low = jnp.where(here, (left & 15).astype(jnp.float32), 0.0)
        both = jnp.concatenate([high, low], axis=0).astype(jnp.bfloat16)
        ids = ids + lax.dot_general(
            hots[i], both, (((1,), (1,)), ((), ())), preferred_element_type=jnp.float32
        )
    ids = ROWS - (16.0 * ids[:, :128] + ids[:, 128:])
    lane = lax.broadcasted_iota(jnp.int32, (OWNERS, 128), 1)
    ids = jnp.where(ids == ROWS, (ROWS + (lane & 15)).astype(jnp.float32), ids)
    ids = jnp.where((lane >> 4) == mine, ids, 0.0)
    for a in range(OWNERS // 8):
        for h in range(2):
            spot = (16 * a + h) * BLOCK + 2 * SLOTS
            send[pl.ds(spot, 8, stride=2 * BLOCK), :] = ids[8 * a : 8 * a + 8]
    lax.fori_loop(2 * PITCH // 64, 2 * PITCH // 32, clear, 0)
    loads[2].wait()
    move.wait()

    def tokens(step, _):
        rows = x_v.at[pl.ds(pl.multiple_of(step * 512, 512), 512)]
        for k in range(128):
            block = dest_s[step, k]
            base = k // 8 * 32 + k % 8
            send[pl.ds(block, 2, stride=SLOTS), :] = rows[pl.ds(base, 2, stride=8), :]
            send[pl.ds(block + BLOCK, 2, stride=SLOTS), :] = rows[pl.ds(base + 16, 2, stride=8), :]
        return 0

    lax.fori_loop(0, TOKENS // 128, tokens, 0)


def pack(owner, row, x):
    return pl.pallas_call(
        pack_kernel,
        out_shape=(jax.ShapeDtypeStruct((DEVICES * BLOCK, 128), jnp.float32),)
        + (jax.ShapeDtypeStruct((2 * PITCH, 128), jnp.float32),) * CHAINS,
        in_specs=[pl.BlockSpec(memory_space=HBM)] * 3,
        out_specs=(pl.BlockSpec(memory_space=VMEM),) * (1 + CHAINS),
        scratch_shapes=[
            pltpu.VMEM((4, 128), jnp.int32),
            pltpu.VMEM((4, 128), jnp.int32),
            pltpu.VMEM((4 * TOKENS, 128), jnp.float32),
            pltpu.VMEM((4, 128), jnp.int32),
            pltpu.SMEM((4, 128), jnp.int32),
            pltpu.SemaphoreType.DMA((4,)),
        ],
        compiler_params=pltpu.CompilerParams(vmem_limit_bytes=20 * 2**20),
        name="pack",
    )(*(pltpu.with_memory_space_constraint(a, HBM) for a in (owner, row, x)))


def sum_kernel(recv, second, *refs):
    half, squares, second_v = refs[CHAINS : CHAINS + 3]
    sums = refs[CHAINS + 3 : 2 * CHAINS + 3]
    ids_v, ids_s, id_sems, sem = refs[2 * CHAINS + 3 :]
    fetch = pltpu.make_async_copy(second, second_v, sem)
    def move(q):
        part = pl.ds(pl.multiple_of(q * 8, 8), 8)
        return pltpu.make_async_copy(ids_v.at[part], ids_s.at[part], id_sems.at[q])

    for g in range(16):
        lines = recv[pl.ds(g * 8 * BLOCK + 2 * SLOTS, 8, stride=BLOCK), :]
        at = g // 4 * 8 + g % 4
        ids_v[at : at + 1, :] = (2 * jnp.sum(lines, axis=0, keepdims=True)).astype(jnp.int32)
        if g % 4 == 3:
            move(g // 4).start()

    fetch.start()

    def add(q, _):
        move(q).wait()
        lines = recv.at[pl.ds(pl.multiple_of(q * 32 * BLOCK, 8), 32 * BLOCK)]
        for at in range(32 * SLOTS):
            total = sums[at % CHAINS]
            line = at // SLOTS * BLOCK + at % SLOTS
            spot = pl.ds(pl.multiple_of(ids_s[q * 8 + at // 128, at % 128], 2), 2)
            total[spot, :] = total[spot, :] + lines[pl.ds(line, 2, stride=SLOTS), :]
        return 0

    lax.fori_loop(0, 4, add, 0)

    def fold(i, squared):
        squared = list(squared)
        for k in range(32):
            at = pl.ds(pl.multiple_of(i * 256 + k * 8, 8), 8)
            parts = [total[at, :] for total in sums]
            while len(parts) > 1:
                parts = [sum(parts[k : k + 2]) for k in range(0, len(parts), 2)]
            half[at, :] = parts[0]
            squared[k % 4] = squared[k % 4] + parts[0] * parts[0]
        return tuple(squared)

    zero = jnp.zeros((8, 128), jnp.float32)
    a, b, c, d = lax.fori_loop(0, ROWS // 128, fold, (zero,) * 4)
    squares[...] = jnp.broadcast_to(jnp.sum((a + b) + (c + d), axis=0, keepdims=True), squares.shape)
    fetch.wait()


def sum_rows(recv, second, sums):
    total = jax.ShapeDtypeStruct((2 * PITCH, 128), jnp.float32)
    return pl.pallas_call(
        sum_kernel,
        out_shape=(
            jax.ShapeDtypeStruct((2 * ROWS, 128), jnp.float32),
            jax.ShapeDtypeStruct((DEVICES, 128), jnp.float32),
            jax.ShapeDtypeStruct((ROWS // 8, 4, 8, 128), jnp.float32),
        )
        + (total,) * CHAINS,
        in_specs=[pl.BlockSpec(memory_space=VMEM), pl.BlockSpec(memory_space=HBM)]
        + [pl.BlockSpec(memory_space=VMEM)] * CHAINS,
        out_specs=(pl.BlockSpec(memory_space=VMEM),) * (3 + CHAINS),
        scratch_shapes=[
            pltpu.VMEM((32, 128), jnp.int32),
            pltpu.SMEM((32, 128), jnp.int32),
            pltpu.SemaphoreType.DMA((4,)),
            pltpu.SemaphoreType.DMA,
        ],
        input_output_aliases={2 + c: 3 + c for c in range(CHAINS)},
        compiler_params=pltpu.CompilerParams(vmem_limit_bytes=22 * 2**20),
        name="sum_rows",
    )(recv, pltpu.with_memory_space_constraint(second, HBM), *sums)


def update_kernel(part, own, other, table, moment, second, *rest):
    outs, bufs, sems = rest[0:3], rest[3:6], rest[6]
    total = jnp.sum(part[...], keepdims=True)
    limit = 0.5 * float(VOCAB * LW) ** 0.5
    clip = jnp.minimum(1.0, limit / (jnp.sqrt(total) + 1e-06))
    first_fix = 1.0 - 0.9**ADAM_STEP
    second_fix = 1.0 - 0.999**ADAM_STEP
    to_moment = jnp.broadcast_to(0.1 * clip, (8, 128))
    to_second = jnp.broadcast_to(0.001 * clip * clip, (8, 128))
    rep = lax.axis_index("rep")

    def tile(i, _):
        rows = pl.ds(i * 4, 4)
        for h, source in enumerate((own, other)):
            cols = pl.ds(jnp.where(rep == 0, h, 1 - h) * 2, 2)
            ins = [ref.at[rows, cols] for ref in (table, moment, second)]
            to = [ref.at[rows, cols] for ref in bufs]
            grads = source.at[pl.ds(pl.multiple_of(i * 64, 64), 64)]
            for k in range(4):
                for j in range(2):
                    g = grads[pl.ds(k * 16 + j, 8, stride=2), :]
                    nm = 0.9 * ins[1][k, j] + to_moment * g
                    nv = 0.999 * ins[2][k, j] + to_second * (g * g)
                    root = (nv * lax.rsqrt(nv)) * (1.0 / second_fix) ** 0.5 + 1e-08
                    to[1][k, j] = nm
                    to[2][k, j] = nv
                    step = (nm * (0.01 / first_fix)) / root
                    to[0][k, j] = (1.0 - 0.0001) * ins[0][k, j] - step
        return 0

    def copies(c, first):
        rows = pl.ds(first, CHUNKS[c])
        return [
            pltpu.make_async_copy(buf.at[rows], out.at[rows], sems.at[n, c])
            for n, (buf, out) in enumerate(zip(bufs, outs))
        ]

    first = 0
    started = []
    for c, count in enumerate(CHUNKS):
        lax.fori_loop(first // 4, (first + count) // 4, tile, 0)
        chunk = copies(c, first)
        for copy in chunk:
            copy.start()
        started += chunk
        first += count
    for copy in started:
        copy.wait()


def update(part, own, other, table, moment, second):
    shape = jax.ShapeDtypeStruct((ROWS // 8, 4, 8, 128), jnp.float32)
    return pl.pallas_call(
        update_kernel,
        out_shape=(shape,) * 3,
        in_specs=[pl.BlockSpec(memory_space=VMEM)] * 6,
        out_specs=(pl.BlockSpec(memory_space=pl.ANY),) * 3,
        scratch_shapes=[pltpu.VMEM((ROWS // 8, 4, 8, 128), jnp.float32)] * 3
        + [pltpu.SemaphoreType.DMA((3, len(CHUNKS)))],
        compiler_params=pltpu.CompilerParams(vmem_limit_bytes=30 * 2**20),
        name="update",
    )(part, own, other, table, moment, second)


def tiles(array):
    rows, cols = array.shape
    return array.reshape(rows // 8, 8, cols // 128, 128).transpose(0, 2, 1, 3)


def local(row_grads, token_owner, token_row, table, moment, second):
    x = tiles(row_grads).reshape(4 * TOKENS, 128)
    send, *sums = pack(token_owner.reshape(4, 128), token_row.reshape(4, 128), x)
    recv = lax.all_to_all(send.reshape(DEVICES, 1, BLOCK * 128), AXES, 0, 0, tiled=True)
    lines = recv.reshape(DEVICES * BLOCK, 128)
    half, squares, second = sum_rows(lines, tiles(second), sums)[:3]
    part = lax.all_to_all(squares.reshape(DEVICES, 1, 128), AXES, 0, 0, tiled=True)
    other = lax.ppermute(half, "rep", [(0, 1), (1, 0)])
    outs = update(part.reshape(DEVICES, 128), half, other, tiles(table), tiles(moment), second)
    return tuple(out.transpose(0, 2, 1, 3).reshape(ROWS, LW) for out in outs)


def solution(mesh):
    return jax.shard_map(
        local,
        mesh=mesh,
        in_specs=(
            P(("dp", "rep"), None),
            P(("dp", "rep"), None),
            P(("dp", "rep")),
            P("dp", None),
            P("dp", None),
            P("dp", None),
        ),
        out_specs=(P("dp", None), P("dp", None), P("dp", None)),
        check_vma=False,
    )
```

```python
import jax
import jax.numpy as jnp
from jax import lax
from jax.experimental import pallas as pl
from jax.experimental.pallas import tpu as pltpu
from jax.sharding import PartitionSpec as P

VOCAB = 131072
ADAM_STEP = 100
LW = 512
OWNERS = 64
SLOTS = 16
TOKENS = 512
ROWS = 2048
DEVICES = 128
BLOCK = 2 * SLOTS + 1
PITCH = 2064
CHAINS = 6
CHUNKS = (12, 16, 20, 28, 36, 48, 60, 36)
AXES = ("dp", "rep")
VMEM = pltpu.MemorySpace.VMEM
SMEM = pltpu.MemorySpace.SMEM
HBM = pltpu.MemorySpace.HBM


def pack_kernel(owner, row, x, send, *refs):
    sums = refs[:CHAINS]
    owner_v, row_v, x_v, dest_v, dest_s, sems = refs[CHAINS:]
    loads = [
        pltpu.make_async_copy(a, b, sems.at[n])
        for n, (a, b) in enumerate(((owner, owner_v), (row, row_v), (x, x_v)))
    ]
    for load in loads:
        load.start()
    early = lax.broadcasted_iota(jnp.int32, (128, 128), 0)
    late = lax.broadcasted_iota(jnp.int32, (128, 128), 1)
    before = jnp.where(early < late, 1.0, 0.0).astype(jnp.bfloat16)
    ones = jnp.ones((128, 128), jnp.bfloat16)
    who = lax.broadcasted_iota(jnp.int32, (OWNERS, 128), 0)
    base = (who * (2 * BLOCK)).astype(jnp.float32)
    mine = lax.rem(lax.axis_index("dp") * 2 + lax.axis_index("rep"), 8)

    def clear(i, _):
        for total in sums:
            for k in range(4):
                total[pl.ds(i * 32 + k * 8, 8), :] = jnp.zeros((8, 128), jnp.float32)
        return 0

    lax.fori_loop(0, 86, clear, 0)
    loads[0].wait()
    masks = [who == owner_v[i : i + 1, :] for i in range(4)]
    hots = [jnp.where(mask, 1.0, 0.0).astype(jnp.bfloat16) for mask in masks]
    hot = jnp.concatenate(hots, axis=0)
    inside = jnp.dot(hot, before, preferred_element_type=jnp.float32)
    counts = jnp.dot(hot, ones, preferred_element_type=jnp.float32)
    seen = jnp.zeros((OWNERS, 128), jnp.float32)
    positions = []
    for i in range(4):
        part = slice(i * OWNERS, (i + 1) * OWNERS)
        at = jnp.where(masks[i], inside[part] + seen, 0.0)
        positions.append(jnp.sum(at, axis=0, keepdims=True))
        start = jnp.sum(jnp.where(masks[i], base, 0.0), axis=0, keepdims=True)
        dest_v[i : i + 1, :] = (start + positions[i]).astype(jnp.int32)
        seen = seen + counts[part]
    move = pltpu.make_async_copy(dest_v, dest_s, sems.at[3])
    move.start()
    loads[1].wait()
    lines = early - mine * SLOTS
    ids = jnp.zeros((OWNERS, 256), jnp.float32)
    for i in range(4):
        left = ROWS - row_v[i : i + 1, :]
        here = lines == positions[i].astype(jnp.int32)
        high = jnp.where(here, (left >> 4).astype(jnp.float32), 0.0)
        low = jnp.where(here, (left & 15).astype(jnp.float32), 0.0)
        both = jnp.concatenate([high, low], axis=0).astype(jnp.bfloat16)
        ids = ids + lax.dot_general(
            hots[i], both, (((1,), (1,)), ((), ())), preferred_element_type=jnp.float32
        )
    ids = ROWS - (16.0 * ids[:, :128] + ids[:, 128:])
    lane = lax.broadcasted_iota(jnp.int32, (OWNERS, 128), 1)
    ids = jnp.where(ids == ROWS, (ROWS + (lane & 15)).astype(jnp.float32), ids)
    ids = jnp.where((lane >> 4) == mine, ids, 0.0)
    for a in range(OWNERS // 8):
        for h in range(2):
            spot = (16 * a + h) * BLOCK + 2 * SLOTS
            send[pl.ds(spot, 8, stride=2 * BLOCK), :] = ids[8 * a : 8 * a + 8]
    lax.fori_loop(86, 2 * PITCH // 32, clear, 0)
    loads[2].wait()
    move.wait()

    def tokens(step, _):
        rows = x_v.at[pl.ds(pl.multiple_of(step * 512, 512), 512)]
        for k in range(128):
            block = dest_s[step, k]
            base = k // 8 * 32 + k % 8
            send[pl.ds(block, 2, stride=SLOTS), :] = rows[pl.ds(base, 2, stride=8), :]
            send[pl.ds(block + BLOCK, 2, stride=SLOTS), :] = rows[pl.ds(base + 16, 2, stride=8), :]
        return 0

    lax.fori_loop(0, TOKENS // 128, tokens, 0)


def pack(owner, row, x):
    return pl.pallas_call(
        pack_kernel,
        out_shape=(jax.ShapeDtypeStruct((DEVICES * BLOCK, 128), jnp.float32),)
        + (jax.ShapeDtypeStruct((2 * PITCH, 128), jnp.float32),) * CHAINS,
        in_specs=[pl.BlockSpec(memory_space=HBM)] * 3,
        out_specs=(pl.BlockSpec(memory_space=VMEM),) * (1 + CHAINS),
        scratch_shapes=[
            pltpu.VMEM((4, 128), jnp.int32),
            pltpu.VMEM((4, 128), jnp.int32),
            pltpu.VMEM((4 * TOKENS, 128), jnp.float32),
            pltpu.VMEM((4, 128), jnp.int32),
            pltpu.SMEM((4, 128), jnp.int32),
            pltpu.SemaphoreType.DMA((4,)),
        ],
        compiler_params=pltpu.CompilerParams(vmem_limit_bytes=20 * 2**20),
        name="pack",
    )(*(pltpu.with_memory_space_constraint(a, HBM) for a in (owner, row, x)))


def sum_kernel(recv, *refs):
    half, squares = refs[CHAINS : CHAINS + 2]
    sums = refs[CHAINS + 2 : 2 * CHAINS + 2]
    ids_v, ids_s, id_sems = refs[2 * CHAINS + 2 :]
    def move(q):
        part = pl.ds(pl.multiple_of(q * 8, 8), 8)
        return pltpu.make_async_copy(ids_v.at[part], ids_s.at[part], id_sems.at[q])

    for g in range(16):
        lines = recv[pl.ds(g * 8 * BLOCK + 2 * SLOTS, 8, stride=BLOCK), :]
        at = g // 4 * 8 + g % 4
        ids_v[at : at + 1, :] = (2 * jnp.sum(lines, axis=0, keepdims=True)).astype(jnp.int32)
        if g % 4 == 3:
            move(g // 4).start()


    def add(q, _):
        move(q).wait()
        lines = recv.at[pl.ds(pl.multiple_of(q * 32 * BLOCK, 8), 32 * BLOCK)]
        for at in range(32 * SLOTS):
            total = sums[at % CHAINS]
            line = at // SLOTS * BLOCK + at % SLOTS
            spot = pl.ds(pl.multiple_of(ids_s[q * 8 + at // 128, at % 128], 2), 2)
            total[spot, :] = total[spot, :] + lines[pl.ds(line, 2, stride=SLOTS), :]
        return 0

    lax.fori_loop(0, 4, add, 0)

    def fold(i, squared):
        squared = list(squared)
        for k in range(32):
            at = pl.ds(pl.multiple_of(i * 256 + k * 8, 8), 8)
            parts = [total[at, :] for total in sums]
            while len(parts) > 1:
                parts = [sum(parts[k : k + 2]) for k in range(0, len(parts), 2)]
            half[at, :] = parts[0]
            squared[k % 4] = squared[k % 4] + parts[0] * parts[0]
        return tuple(squared)

    zero = jnp.zeros((8, 128), jnp.float32)
    a, b, c, d = lax.fori_loop(0, ROWS // 128, fold, (zero,) * 4)
    squares[...] = jnp.broadcast_to(jnp.sum((a + b) + (c + d), axis=0, keepdims=True), squares.shape)


def sum_rows(recv, sums):
    total = jax.ShapeDtypeStruct((2 * PITCH, 128), jnp.float32)
    return pl.pallas_call(
        sum_kernel,
        out_shape=(
            jax.ShapeDtypeStruct((2 * ROWS, 128), jnp.float32),
            jax.ShapeDtypeStruct((DEVICES, 128), jnp.float32),
        )
        + (total,) * CHAINS,
        in_specs=[pl.BlockSpec(memory_space=VMEM)] * (1 + CHAINS),
        out_specs=(pl.BlockSpec(memory_space=VMEM),) * (2 + CHAINS),
        scratch_shapes=[
            pltpu.VMEM((32, 128), jnp.int32),
            pltpu.SMEM((32, 128), jnp.int32),
            pltpu.SemaphoreType.DMA((4,)),
        ],
        input_output_aliases={1 + c: 2 + c for c in range(CHAINS)},
        compiler_params=pltpu.CompilerParams(vmem_limit_bytes=22 * 2**20),
        name="sum_rows",
    )(recv, *sums)


def update_kernel(part, own, other, table, moment, second, *rest):
    outs, bufs, sems = rest[0:3], rest[3:6], rest[6]
    total = jnp.sum(part[...], keepdims=True)
    limit = 0.5 * float(VOCAB * LW) ** 0.5
    clip = jnp.minimum(1.0, limit / (jnp.sqrt(total) + 1e-06))
    first_fix = 1.0 - 0.9**ADAM_STEP
    second_fix = 1.0 - 0.999**ADAM_STEP
    to_moment = jnp.broadcast_to(0.1 * clip, (8, 128))
    to_second = jnp.broadcast_to(0.001 * clip * clip, (8, 128))
    rep = lax.axis_index("rep")

    def tile(i, _):
        rows = pl.ds(i * 4, 4)
        for h, source in enumerate((own, other)):
            cols = pl.ds(jnp.where(rep == 0, h, 1 - h) * 2, 2)
            ins = [ref.at[rows, cols] for ref in (table, moment, second)]
            to = [ref.at[rows, cols] for ref in bufs]
            grads = source.at[pl.ds(pl.multiple_of(i * 64, 64), 64)]
            for k in range(4):
                for j in range(2):
                    g = grads[pl.ds(k * 16 + j, 8, stride=2), :]
                    nm = 0.9 * ins[1][k, j] + to_moment * g
                    nv = 0.999 * ins[2][k, j] + to_second * (g * g)
                    root = (nv * lax.rsqrt(nv)) * (1.0 / second_fix) ** 0.5 + 1e-08
                    to[1][k, j] = nm
                    to[2][k, j] = nv
                    step = (nm * (0.01 / first_fix)) / root
                    to[0][k, j] = (1.0 - 0.0001) * ins[0][k, j] - step
        return 0

    def copies(c, first):
        rows = pl.ds(first, CHUNKS[c])
        return [
            pltpu.make_async_copy(buf.at[rows], out.at[rows], sems.at[n, c])
            for n, (buf, out) in enumerate(zip(bufs, outs))
        ]

    first = 0
    started = []
    for c, count in enumerate(CHUNKS):
        lax.fori_loop(first // 4, (first + count) // 4, tile, 0)
        chunk = copies(c, first)
        for copy in chunk:
            copy.start()
        started += chunk
        first += count
    for copy in started:
        copy.wait()


def update(part, own, other, table, moment, second):
    shape = jax.ShapeDtypeStruct((ROWS // 8, 4, 8, 128), jnp.float32)
    return pl.pallas_call(
        update_kernel,
        out_shape=(shape,) * 3,
        in_specs=[pl.BlockSpec(memory_space=VMEM)] * 6,
        out_specs=(pl.BlockSpec(memory_space=pl.ANY),) * 3,
        scratch_shapes=[pltpu.VMEM((ROWS // 8, 4, 8, 128), jnp.float32)] * 3
        + [pltpu.SemaphoreType.DMA((3, len(CHUNKS)))],
        compiler_params=pltpu.CompilerParams(vmem_limit_bytes=30 * 2**20),
        name="update",
    )(part, own, other, table, moment, second)


def tiles(array):
    rows, cols = array.shape
    return array.reshape(rows // 8, 8, cols // 128, 128).transpose(0, 2, 1, 3)


def local(row_grads, token_owner, token_row, table, moment, second):
    x = tiles(row_grads).reshape(4 * TOKENS, 128)
    send, *sums = pack(token_owner.reshape(4, 128), token_row.reshape(4, 128), x)
    recv = lax.all_to_all(send.reshape(DEVICES, 1, BLOCK * 128), AXES, 0, 0, tiled=True)
    lines = recv.reshape(DEVICES * BLOCK, 128)
    half, squares = sum_rows(lines, sums)[:2]
    part = lax.all_to_all(squares.reshape(DEVICES, 1, 128), AXES, 0, 0, tiled=True)
    other = lax.ppermute(half, "rep", [(0, 1), (1, 0)])
    outs = update(part.reshape(DEVICES, 128), half, other, tiles(table), tiles(moment), tiles(second))
    return tuple(out.transpose(0, 2, 1, 3).reshape(ROWS, LW) for out in outs)


def solution(mesh):
    return jax.shard_map(
        local,
        mesh=mesh,
        in_specs=(
            P(("dp", "rep"), None),
            P(("dp", "rep"), None),
            P(("dp", "rep")),
            P("dp", None),
            P("dp", None),
            P("dp", None),
        ),
        out_specs=(P("dp", None), P("dp", None), P("dp", None)),
        check_vma=False,
    )
```
